32 devices in a mesh: row: 8 (over z, x), col: 4 (over y, core).
Axes of the slice: x: 2, y: 2, z: 4, core: 2. Of those that a mesh axis runs over, the one named last changes fastest.
Arguments:
- state: bfloat16 [256, 16384], P(None, ('row', 'col')), may hold values from -0.94921875 to 0.94921875
- adjoint: bfloat16 [256, 16384], P(None, ('col', 'row')), may hold values from -6 to 6
- features: bfloat16 [128, 16384], P(None, ('col', 'row')), may hold values from -6 to 6
- cotangent: bfloat16 [256, 16384], P(None, ('row', 'col')), may hold values from -6 to 6
- mixing: bfloat16 [256, 256], replicated, may hold values from -0.375 to 0.375
- input_weight: bfloat16 [256, 128], replicated, may hold values from -0.5 to 0.5
- tiles: bfloat16 [8, 4, 170, 128, 128], P('row', 'col'), may hold values from -0.09375 to 0.09375
- tile_rows: int32 [8, 4, 170], P('row', 'col'), may hold values from 0 to 15, as said below
- tile_cols: int32 [8, 4, 170], P('row', 'col'), may hold values from 0 to 31, as said below
- live_tiles: int32 [8, 4], P('row', 'col'), may hold values from 85 to 170, as said below
Outputs:
- new_state: bfloat16 [256, 16384], P(None, ('col', 'row'))
- new_adjoint: bfloat16 [256, 16384], P(None, ('row', 'col'))
The draws below stay inside these ranges and needn't reach their ends.
Inputs may be any that keep to these rules, and one draw needn't show every extreme that they name: On one device the pairs (tile_rows, tile_cols) of its 170 slots are all different. `tile_cols`: see tile_rows. `live_tiles`: some device has all 170 slots live.
All inputs are finite; a program needn't handle non-finite values.
Results may differ from the reference program's by a relative error of at most 0.014.
Values may be sent and summed in bfloat16 or wider, within the bound.
No kernel may reach another device: no remote copies, remote signals or barrier semaphores. Data moves between devices by JAX's collectives and lax.ppermute only.
A program may use at most 64 MiB of HBM per device.

```python
import jax
import jax.numpy as jnp
from jax import lax

H = 256
F = 128
TILE = 128
BR = 16
BC = 32
N = 16384
CAP = 170
N_ROW = 8
N_COL = 4


def pattern(key):
    row_count = N // (BR * TILE)
    col_count = N // (BC * TILE)
    total = BR * BC
    first_key = jax.random.fold_in(key, 101)
    second_key = jax.random.fold_in(key, 202)
    third_key = jax.random.fold_in(key, 303)
    scores = jax.random.randint(first_key, (row_count, col_count, total), 0, 2 ** 30 // total, dtype=jnp.int32)
    scores = scores * total + jnp.arange(total, dtype=jnp.int32)
    chosen = jnp.argsort(scores, axis=-1)[..., :CAP].astype(jnp.int32)
    rows_drawn = chosen // BC
    cols_drawn = chosen % BC
    counts = jax.random.randint(second_key, (row_count, col_count), CAP // 2, CAP + 1, dtype=jnp.int32)
    fullest = jax.random.randint(third_key, (), 0, row_count * col_count, dtype=jnp.int32)
    places = jnp.arange(row_count * col_count, dtype=jnp.int32).reshape(row_count, col_count)
    counts = jnp.where(places == fullest, CAP, counts)
    return (rows_drawn, cols_drawn, counts)


def draw_tile_rows(key, part):
    return pattern(key)[0].astype(jnp.int32)


def draw_tile_cols(key, part):
    return pattern(key)[1].astype(jnp.int32)


def draw_live_tiles(key, part):
    return pattern(key)[2].astype(jnp.int32)


def levels(stream_key, dims, split, smallest, high):
    factor_of, own = 1.0, jax.random.fold_in(stream_key, 6)
    for position, blocks in split:
        draws = jnp.exp(jax.random.uniform(jax.random.fold_in(own, position), (blocks,), jnp.float32, smallest / len(split), high / len(split)))
        factor_of = factor_of * jnp.repeat(draws, dims[position] // blocks).reshape([-1 if axis == position else 1 for axis in range(len(dims))])
    return factor_of


def scatter_about(rng, shape, spread, reach, shards=(), kind=jnp.bfloat16):
    array = jax.random.normal(rng, shape, jnp.float32) * spread
    if len(shards) > 0:
        array = levels(rng, shape, shards, -0.22, 0.18) * array
    return jnp.clip(array, min=-reach, max=reach).astype(kind)


def setup_inputs(seed: int = 0) -> dict:
    arg_keys = jax.random.split(jax.random.key(seed), 11)
    return {
        "state": jnp.clip(jax.random.uniform(arg_keys[0], (H, N), jnp.float32, -0.94921875, 0.94921875) * levels(arg_keys[0], (H, N), ((1, 32),), -0.4, 0.0), -0.94921875, 0.94921875).astype(jnp.bfloat16),
        "adjoint": scatter_about(arg_keys[1], (H, N), 1.0, 6.0, ((1, 32),)),
        "features": scatter_about(arg_keys[2], (F, N), 1.0, 6.0, ((1, 32),)),
        "cotangent": scatter_about(arg_keys[3], (H, N), 1.0, 6.0, ((1, 32),)),
        "mixing": scatter_about(arg_keys[4], (H, H), H ** -0.5, 0.375),
        "input_weight": scatter_about(arg_keys[5], (H, F), F ** -0.5, 0.5),
        "tiles": scatter_about(arg_keys[6], (N_ROW, N_COL, CAP, TILE, TILE), (N // 4) ** -0.5, 0.09375, ((0, 8), (1, 4))),
        "tile_rows": draw_tile_rows(jax.random.fold_in(arg_keys[10], 71), 0),
        "tile_cols": draw_tile_cols(jax.random.fold_in(arg_keys[10], 71), 0),
        "live_tiles": draw_live_tiles(jax.random.fold_in(arg_keys[10], 71), 0),
    }


def round_half(values):
    narrow = values.astype(jnp.bfloat16)
    narrow = lax.optimization_barrier(narrow)
    return narrow.astype(jnp.float32)


def reference(state, adjoint, features, cotangent, mixing, input_weight, tiles, tile_rows, tile_cols, live_tiles):
    hidden = state.shape[0]
    width_rows = BR * TILE
    width_cols = BC * TILE
    state_wide = state.astype(jnp.float32)
    adjoint_wide = adjoint.astype(jnp.float32)

    def device_step(index, carry):
        forward_sum, backward_sum = carry
        index = index.astype(jnp.int32)
        row_index = index // N_COL
        col_index = index % N_COL
        block_tiles = tiles[row_index, col_index].astype(jnp.float32)
        rows_here = tile_rows[row_index, col_index]
        cols_here = tile_cols[row_index, col_index]
        live = (jnp.arange(CAP, dtype=jnp.int32) < live_tiles[row_index, col_index]).astype(jnp.float32)
        row_start = (row_index * width_rows).astype(jnp.int32)
        col_start = (col_index * width_cols).astype(jnp.int32)
        state_part = lax.dynamic_slice_in_dim(state_wide, row_start, width_rows, 1).reshape(hidden, BR, TILE)
        adjoint_part = lax.dynamic_slice_in_dim(adjoint_wide, col_start, width_cols, 1).reshape(hidden, BC, TILE)
        chosen_state = jnp.take(state_part, rows_here, axis=1)
        forward_terms = jnp.einsum("hsk,skn->hsn", chosen_state, block_tiles, precision=lax.Precision.HIGHEST)
        forward_terms = forward_terms * live[None, :, None]
        forward_local = jnp.zeros((hidden, BC, TILE), jnp.float32).at[:, cols_here].add(forward_terms)
        chosen_adjoint = jnp.take(adjoint_part, cols_here, axis=1)
        backward_terms = jnp.einsum("hsn,skn->hsk", chosen_adjoint, block_tiles, precision=lax.Precision.HIGHEST)
        backward_terms = backward_terms * live[None, :, None]
        backward_local = jnp.zeros((hidden, BR, TILE), jnp.float32).at[:, rows_here].add(backward_terms)
        forward_local = round_half(forward_local)
        backward_local = round_half(backward_local)
        forward_old = lax.dynamic_slice_in_dim(forward_sum, col_start, width_cols, 1)
        forward_sum = lax.dynamic_update_slice_in_dim(forward_sum, forward_old + forward_local.reshape(hidden, width_cols), col_start, 1)
        backward_old = lax.dynamic_slice_in_dim(backward_sum, row_start, width_rows, 1)
        backward_sum = lax.dynamic_update_slice_in_dim(backward_sum, backward_old + backward_local.reshape(hidden, width_rows), row_start, 1)
        return forward_sum, backward_sum

    empty = jnp.zeros((hidden, N), jnp.float32)
    forward_sum, backward_sum = lax.fori_loop(0, N_ROW * N_COL, device_step, (empty, empty))
    flow = forward_sum.astype(jnp.bfloat16)
    pre = jnp.dot(mixing, flow, preferred_element_type=jnp.float32) + jnp.dot(input_weight, features, preferred_element_type=jnp.float32)
    new_state = jnp.tanh(pre).astype(jnp.bfloat16)
    back = backward_sum.astype(jnp.bfloat16)
    slope = 1.0 - state_wide * state_wide
    new_adjoint = (slope * (jnp.dot(mixing.T, back, preferred_element_type=jnp.float32) + cotangent.astype(jnp.float32))).astype(jnp.bfloat16)
    return new_state, new_adjoint
```

```python
import functools

import jax
import jax.numpy as jnp
from jax import lax
from jax.experimental import pallas as pl
from jax.experimental.pallas import tpu as pltpu
from jax.sharding import PartitionSpec as P


VMEM = pltpu.VMEM
BF16 = jnp.bfloat16
F32 = jnp.float32
NT = (((1,), (1,)), ((), ()))


def in_vmem():
    return pl.BlockSpec(memory_space=VMEM)


def swap(value, axis, size, mask):
    return lax.ppermute(value, axis, [(i, i ^ mask) for i in range(size)])


def build_kernel(group, rows, cols, count, tiles, dense):
    step = pl.program_id(0)
    side = tiles.shape[-1]
    height = dense.shape[0]

    @pl.when(step == 0)
    def _():
        def clear(i, carry):
            dense[pl.ds(pl.multiple_of(i * 32, 32), 32), :] = jnp.zeros((32, dense.shape[1]), dense.dtype)
            return carry

        lax.fori_loop(0, height // 32, clear, 0)

    def place(i, carry):
        slot = step * group + i
        r = pl.multiple_of(rows[slot] * side, side)
        c = pl.multiple_of(cols[slot] * side, side)
        dense[pl.ds(r, side), pl.ds(c, side)] = tiles[i]
        return carry

    lax.fori_loop(0, jnp.clip(count[0] - step * group, 0, group), place, 0)


def build(rows, cols, count, tiles, height, width):
    slots, side, _ = tiles.shape
    group = max(g for g in range(1, 33) if slots % g == 0)
    return pl.pallas_call(
        functools.partial(build_kernel, group),
        grid_spec=pltpu.PrefetchScalarGridSpec(
            num_scalar_prefetch=3,
            grid=(slots // group,),
            in_specs=[pl.BlockSpec((group, side, side), lambda i, *_: (i, 0, 0))],
            out_specs=in_vmem(),
        ),
        out_shape=jax.ShapeDtypeStruct((height, width), BF16),
        compiler_params=pltpu.CompilerParams(vmem_limit_bytes=24 * 2**20),
        cost_estimate=pl.CostEstimate(flops=5 * 10**9, bytes_accessed=tiles.size * 2, transcendentals=0),
        name="build",
    )(rows, cols, count, tiles)


def forward_kernel(parts, *refs):
    blocks, dense, outs, whole = refs[:parts], refs[parts], refs[parts + 1 : -1], refs[-1]
    width = blocks[0].shape[1]
    for k in range(parts):
        whole[:, k * width : (k + 1) * width] = blocks[k][...]
    span = outs[0].shape[1]
    for j, out in enumerate(outs):
        out[...] = jnp.dot(
            whole[...], dense[:, j * span : (j + 1) * span], preferred_element_type=F32
        ).astype(BF16)


def backward_kernel(parts, *refs):
    blocks, dense, outs, whole = refs[:parts], refs[parts], refs[parts + 1 : -1], refs[-1]
    width = blocks[0].shape[1]
    for k in range(parts):
        whole[:, k * width : (k + 1) * width] = blocks[k][...]
    span = outs[0].shape[1]
    for j, out in enumerate(outs):
        out[...] = lax.dot_general(
            whole[...], dense[j * span : (j + 1) * span, :], NT, preferred_element_type=F32
        ).astype(BF16)


def multiply(kernel, blocks, dense, pieces, name):
    hidden, width = blocks[0].shape
    parts = len(blocks)
    span = (dense.size // (parts * width)) // pieces
    return pl.pallas_call(
        functools.partial(kernel, parts),
        in_specs=[in_vmem()] * (parts + 1),
        out_specs=[in_vmem()] * pieces,
        out_shape=[jax.ShapeDtypeStruct((hidden, span), BF16)] * pieces,
        scratch_shapes=[VMEM((hidden, parts * width), BF16)],
        compiler_params=pltpu.CompilerParams(vmem_limit_bytes=40 * 2**20),
        cost_estimate=pl.CostEstimate(flops=2 * hidden * dense.size, bytes_accessed=dense.size * 2, transcendentals=0),
        name=name,
    )(*blocks, dense)


def state_kernel(terms, *refs):
    flow = refs[0][...].astype(F32)
    for ref in refs[1:terms]:
        flow = flow + ref[...].astype(F32)
    mixing, weight, features, out = refs[terms:]
    pre = jnp.dot(mixing[...], flow.astype(BF16), preferred_element_type=F32)
    pre = pre + jnp.dot(weight[...], features[...], preferred_element_type=F32)
    out[...] = jnp.tanh(pre).astype(BF16)


def adjoint_kernel(terms, *refs):
    back = refs[0][...].astype(F32)
    for ref in refs[1:terms]:
        back = back + ref[...].astype(F32)
    mixing_t, state, cotangent, out = refs[terms:]
    pulled = jnp.dot(mixing_t[...], back.astype(BF16), preferred_element_type=F32)
    wide = state[...].astype(F32)
    out[...] = ((1.0 - wide * wide) * (pulled + cotangent[...].astype(F32))).astype(BF16)


def finish(kernel, terms, others, name):
    return pl.pallas_call(
        functools.partial(kernel, len(terms)),
        in_specs=[in_vmem()] * (len(terms) + len(others)),
        out_specs=in_vmem(),
        out_shape=jax.ShapeDtypeStruct(terms[0].shape, BF16),
        compiler_params=pltpu.CompilerParams(vmem_limit_bytes=16 * 2**20),
        cost_estimate=pl.CostEstimate(flops=10**9, bytes_accessed=2**21, transcendentals=0),
        name=name,
    )(*terms, *others)


def per_device(state, adjoint, features, cotangent, mixing, input_weight, tiles, tile_rows, tile_cols, live_tiles):
    n_row, n_col = lax.axis_size("row"), lax.axis_size("col")
    my_row, my_col = lax.axis_index("row"), lax.axis_index("col")
    hidden, nodes = state.shape
    slab = tiles[0, 0]
    side = slab.shape[-1]
    per_chunk = nodes // side
    rows = tile_rows[0, 0]
    cols = tile_cols[0, 0]
    rows = ((rows // per_chunk) ^ my_col) * per_chunk + rows % per_chunk
    cols = ((cols // per_chunk) ^ my_row) * per_chunk + cols % per_chunk

    states = [state] + [swap(state, "col", n_col, k) for k in range(1, n_col)]
    near = [adjoint] + [swap(adjoint, "row", n_row, 2 * k) for k in range(1, n_row // 2)]
    adjoints = []
    for block in near:
        adjoints += [block, swap(block, "row", n_row, 1)]

    dense = build(rows, cols, live_tiles[0], slab, n_col * nodes, n_row * nodes)

    shares = multiply(forward_kernel, states, dense, n_row, "forward")
    flows = []
    for k in range(n_row // 2):
        mine, other = shares[2 * k], swap(shares[2 * k + 1], "row", n_row, 1)
        if k:
            pair = (mine.astype(F32) + other.astype(F32)).astype(BF16)
            flows.append(swap(pair, "row", n_row, 2 * k))
        else:
            flows += [mine, other]
    new_state = finish(state_kernel, flows, (mixing, input_weight, features), "advance")

    shares = multiply(backward_kernel, adjoints, dense, n_col, "backward")
    backs = [shares[0]] + [swap(shares[k], "col", n_col, k) for k in range(1, n_col)]
    new_adjoint = finish(adjoint_kernel, backs, (mixing.T, state, cotangent), "pull")
    return (new_state, new_adjoint)


def solution(mesh):
    placed = (
        P(None, ("row", "col")),
        P(None, ("col", "row")),
        P(None, ("col", "row")),
        P(None, ("row", "col")),
        P(),
        P(),
        P("row", "col", None, None, None),
        P("row", "col", None),
        P("row", "col", None),
        P("row", "col"),
    )
    return jax.shard_map(
        per_device,
        mesh=mesh,
        in_specs=placed,
        out_specs=(P(None, ("col", "row")), P(None, ("row", "col"))),
        check_vma=False,
    )
```

```python
import functools

import jax
import jax.numpy as jnp
from jax import lax
from jax.experimental import pallas as pl
from jax.experimental.pallas import tpu as pltpu
from jax.sharding import PartitionSpec as P


VMEM = pltpu.VMEM
BF16 = jnp.bfloat16
F32 = jnp.float32
NT = (((1,), (1,)), ((), ()))
TN = (((0,), (0,)), ((), ()))


def in_vmem():
    return pl.BlockSpec(memory_space=VMEM)


def swap(value, axis, size, mask):
    return lax.ppermute(value, axis, [(i, i ^ mask) for i in range(size)])


def build_kernel(groups, here, rows, cols, count, tiles, dense, held, sems):
    slots, side, _ = held.shape
    group = slots // groups
    height, width = dense.shape

    def fetch(g):
        part = pl.ds(g * group, group)
        return pltpu.make_async_copy(tiles.at[part], held.at[part], sems.at[g])

    for g in range(groups):
        fetch(g).start()

    def clear(i, carry):
        dense[pl.ds(pl.multiple_of(i * 32, 32), 32), :] = jnp.zeros((32, width), dense.dtype)
        return carry

    lax.fori_loop(0, height // 32, clear, 0)

    def place(slot, carry):
        r, c = rows[slot], cols[slot]
        r = pl.multiple_of((r ^ here[1]) * side, side)
        c = pl.multiple_of((c ^ here[0]) * side, side)
        dense[pl.ds(r, side), pl.ds(c, side)] = held[slot]
        return carry

    for g in range(groups):
        fetch(g).wait()
        lax.fori_loop(g * group, jnp.clip(count[0], g * group, (g + 1) * group), place, 0)


def build(here, rows, cols, count, tiles, height, width):
    slots = tiles.shape[0]
    groups = max(g for g in range(1, 11) if slots % g == 0)
    smem = pl.BlockSpec(memory_space=pltpu.SMEM)
    return pl.pallas_call(
        functools.partial(build_kernel, groups),
        in_specs=[smem] * 4 + [pl.BlockSpec(memory_space=pltpu.HBM)],
        out_specs=in_vmem(),
        out_shape=jax.ShapeDtypeStruct((height, width), BF16),
        scratch_shapes=[VMEM(tiles.shape, BF16), pltpu.SemaphoreType.DMA((groups,))],
        compiler_params=pltpu.CompilerParams(vmem_limit_bytes=8 * 2**20),
        cost_estimate=pl.CostEstimate(flops=5 * 10**9, bytes_accessed=tiles.size * 2, transcendentals=0),
        name="build",
    )(here, rows, cols, count, tiles)


def forward_kernel(parts, extra, *refs):
    blocks, dense, rest = refs[:parts], refs[parts], refs[parts + 1 :]
    picks, rest = rest[:extra], rest[extra:]
    outs, whole = rest[:-1], rest[-1]
    width = blocks[0].shape[1]
    for k in range(parts):
        whole[:, k * width : (k + 1) * width] = blocks[k][...]
    first = 1
    if extra:
        weight, features = picks
        outs[-1][...] = jnp.dot(weight[...], features[...], preferred_element_type=F32)
        outs, first = outs[:-1], 0
    span = outs[0].shape[1]
    for j, out in enumerate(outs):
        start = (2 * j + first) * span
        out[...] = jnp.dot(
            whole[...], dense[:, start : start + span], preferred_element_type=F32
        ).astype(BF16)


def backward_kernel(parts, extra, *refs):
    blocks, dense, rest = refs[:parts], refs[parts], refs[parts + 1 :]
    picks, rest = rest[:extra], rest[extra:]
    outs, whole = rest[:-1], rest[-1]
    width = blocks[0].shape[1]
    for k in range(parts):
        whole[:, k * width : (k + 1) * width] = blocks[k][...]
    first = 0 if extra else 1
    span = outs[0].shape[1]
    for j, out in enumerate(outs):
        start = (2 * j + first) * span
        total = lax.dot_general(
            whole[...], dense[start : start + span, :], NT, preferred_element_type=F32
        )
        if extra and j:
            total = total + picks[j - 1][...].astype(F32)
        out[...] = total.astype(BF16)


def multiply(kernel, blocks, dense, picks, outs):
    hidden, width = blocks[0].shape
    parts = len(blocks)
    return pl.pallas_call(
        functools.partial(kernel, parts, len(picks)),
        in_specs=[in_vmem()] * (parts + 1 + len(picks)),
        out_specs=[in_vmem()] * len(outs),
        out_shape=outs,
        scratch_shapes=[VMEM((hidden, parts * width), BF16)],
        compiler_params=pltpu.CompilerParams(vmem_limit_bytes=8 * 2**20),
        cost_estimate=pl.CostEstimate(flops=hidden * dense.size, bytes_accessed=dense.size, transcendentals=0),
    )(*blocks, dense, *picks)


def state_kernel(terms, *refs):
    flow = refs[0][...].astype(F32)
    for ref in refs[1:terms]:
        flow = flow + ref[...].astype(F32)
    mixing, base, out = refs[terms:]
    pre = base[...] + jnp.dot(mixing[...], flow.astype(BF16), preferred_element_type=F32)
    out[...] = jnp.tanh(pre).astype(BF16)


def adjoint_kernel(terms, *refs):
    back = refs[0][...].astype(F32)
    for ref in refs[1:terms]:
        back = back + ref[...].astype(F32)
    mixing, state, cotangent, out = refs[terms:]
    pulled = lax.dot_general(mixing[...], back.astype(BF16), TN, preferred_element_type=F32)
    wide = state[...].astype(F32)
    out[...] = ((1.0 - wide * wide) * (pulled + cotangent[...].astype(F32))).astype(BF16)


def finish(kernel, terms, others):
    return pl.pallas_call(
        functools.partial(kernel, len(terms)),
        in_specs=[in_vmem()] * (len(terms) + len(others)),
        out_specs=in_vmem(),
        out_shape=jax.ShapeDtypeStruct(terms[0].shape, BF16),
        compiler_params=pltpu.CompilerParams(vmem_limit_bytes=4 * 2**20),
        cost_estimate=pl.CostEstimate(flops=10**9, bytes_accessed=2**21, transcendentals=0),
    )(*terms, *others)


def per_device(state, adjoint, features, cotangent, mixing, input_weight, tiles, tile_rows, tile_cols, live_tiles):
    n_row, n_col = lax.axis_size("row"), lax.axis_size("col")
    my_row, my_col = lax.axis_index("row"), lax.axis_index("col")
    hidden, nodes = state.shape
    slab = tiles[0, 0]
    side = slab.shape[-1]
    per_chunk = nodes // side
    here = jnp.stack([my_row * per_chunk, my_col * per_chunk]).astype(jnp.int32)
    half_row, half_col = n_row // 2, n_col // 2
    piece = jax.ShapeDtypeStruct((hidden, nodes), BF16)
    wide = jax.ShapeDtypeStruct((hidden, nodes), F32)

    def by_row(value, mask):
        return swap(value, "row", n_row, mask)

    def by_col(value, mask):
        return swap(value, "col", n_col, mask)

    near = [adjoint]
    for k in range(1, half_row):
        far = k > 1 and k % 2
        near.append(by_row(near[k - 1] if far else adjoint, 2 if far else 2 * k))
    adjoints = []
    for block in near:
        adjoints += [block, by_row(block, 1)]

    near = [state] + [by_col(state, 2 * k) for k in range(1, half_col)]
    states = []
    for block in near:
        states += [block, by_col(block, 1)]

    dense = build(here, tile_rows[0, 0], tile_cols[0, 0], live_tiles[0], slab, n_col * nodes, n_row * nodes)

    others = multiply(forward_kernel, states, dense, (), [piece] * half_row)
    others = [by_row(others[k], 1) for k in range(half_row)]
    mine = multiply(forward_kernel, states, dense, (input_weight, features), [piece] * half_row + [wide])
    *mine, base = mine
    flows = [mine[0], others[0]]
    relayed = None
    for k in reversed(range(1, half_row)):
        pair = mine[k].astype(F32) + others[k].astype(F32)
        if relayed is not None:
            pair = pair + relayed.astype(F32)
        far = k > 1 and k % 2
        moved = by_row(pair.astype(BF16), 2 if far else 2 * k)
        relayed = moved if far else None
        if not far:
            flows.append(moved)
    new_state = finish(state_kernel, flows, (mixing, base))

    others = multiply(backward_kernel, adjoints, dense, (), [piece] * half_col)
    others = [by_col(others[k], 1) for k in range(half_col)]
    mine = multiply(backward_kernel, adjoints, dense, others[1:], [piece] * half_col)
    backs = [mine[0], others[0]] + [by_col(mine[k], 2 * k) for k in range(1, half_col)]
    new_adjoint = finish(adjoint_kernel, backs, (mixing, state, cotangent))
    return (new_state, new_adjoint)


def solution(mesh):
    placed = (
        P(None, ("row", "col")),
        P(None, ("col", "row")),
        P(None, ("col", "row")),
        P(None, ("row", "col")),
        P(),
        P(),
        P("row", "col", None, None, None),
        P("row", "col", None),
        P("row", "col", None),
        P("row", "col"),
    )
    return jax.shard_map(
        per_device,
        mesh=mesh,
        in_specs=placed,
        out_specs=(P(None, ("col", "row")), P(None, ("row", "col"))),
        check_vma=False,
    )
```

```python
import functools

import jax
import jax.numpy as jnp
from jax import lax
from jax.experimental import pallas as pl
from jax.experimental.pallas import tpu as pltpu
from jax.sharding import PartitionSpec as P


VMEM = pltpu.VMEM
BF16 = jnp.bfloat16
F32 = jnp.float32
NT = (((1,), (1,)), ((), ()))
TN = (((0,), (0,)), ((), ()))


def in_vmem():
    return pl.BlockSpec(memory_space=VMEM)


def swap(value, axis, size, mask):
    return lax.ppermute(value, axis, [(i, i ^ mask) for i in range(size)])


def clear_kernel(dense):
    height, width = dense.shape

    def clear(i, carry):
        dense[pl.ds(pl.multiple_of(i * 32, 32), 32), :] = jnp.zeros((32, width), dense.dtype)
        return carry

    lax.fori_loop(0, height // 32, clear, 0)


def clear(height, width):
    return pl.pallas_call(
        clear_kernel,
        out_specs=in_vmem(),
        out_shape=jax.ShapeDtypeStruct((height, width), BF16),
        compiler_params=pltpu.CompilerParams(vmem_limit_bytes=4 * 2**20),
        cost_estimate=pl.CostEstimate(flops=5 * 10**9, bytes_accessed=height * width * 2, transcendentals=0),
        name="clear",
    )()


def build_kernel(per_chunk, rows, cols, count, tiles, blank, dense):
    slots, side, _ = tiles.shape
    row_flip = lax.axis_index("col") * per_chunk
    col_flip = lax.axis_index("row") * per_chunk

    def place(slot, carry):
        r = pl.multiple_of((rows[0, 0, slot] ^ row_flip) * side, side)
        c = pl.multiple_of((cols[0, 0, slot] ^ col_flip) * side, side)
        dense[pl.ds(r, side), pl.ds(c, side)] = tiles[slot]
        return carry

    lax.fori_loop(0, jnp.clip(count[0, 0], 0, slots), place, 0)


def build(per_chunk, rows, cols, count, tiles, blank):
    smem = pl.BlockSpec(memory_space=pltpu.SMEM)
    return pl.pallas_call(
        functools.partial(build_kernel, per_chunk),
        in_specs=[smem] * 3 + [in_vmem()] * 2,
        out_specs=in_vmem(),
        out_shape=jax.ShapeDtypeStruct(blank.shape, BF16),
        input_output_aliases={4: 0},
        compiler_params=pltpu.CompilerParams(vmem_limit_bytes=4 * 2**20),
        cost_estimate=pl.CostEstimate(flops=5 * 10**9, bytes_accessed=tiles.size * 2, transcendentals=0),
        name="build",
    )(rows, cols, count, tiles, blank)


def forward_kernel(parts, extra, *refs):
    blocks, dense, rest = refs[:parts], refs[parts], refs[parts + 1 :]
    picks, rest = rest[:extra], rest[extra:]
    outs, whole = rest[:-1], rest[-1]
    width = blocks[0].shape[1]
    for k in range(parts):
        whole[:, k * width : (k + 1) * width] = blocks[k][...]
    first = 1
    if extra:
        weight, features = picks
        outs[-1][...] = jnp.dot(weight[...], features[...], preferred_element_type=F32)
        outs, first = outs[:-1], 0
    span = outs[0].shape[1]
    for j, out in enumerate(outs):
        start = (2 * j + first) * span
        out[...] = jnp.dot(
            whole[...], dense[:, start : start + span], preferred_element_type=F32
        ).astype(BF16)


def backward_kernel(parts, extra, *refs):
    blocks, dense, rest = refs[:parts], refs[parts], refs[parts + 1 :]
    picks, rest = rest[:extra], rest[extra:]
    outs, whole = rest[:-1], rest[-1]
    width = blocks[0].shape[1]
    for k in range(parts):
        whole[:, k * width : (k + 1) * width] = blocks[k][...]
    first = 0 if extra else 1
    span = outs[0].shape[1]
    for j, out in enumerate(outs):
        start = (2 * j + first) * span
        total = lax.dot_general(
            whole[...], dense[start : start + span, :], NT, preferred_element_type=F32
        )
        if extra and j:
            total = total + picks[j - 1][...].astype(F32)
        out[...] = total.astype(BF16)


def multiply(kernel, blocks, dense, picks, outs):
    hidden, width = blocks[0].shape
    parts = len(blocks)
    return pl.pallas_call(
        functools.partial(kernel, parts, len(picks)),
        in_specs=[in_vmem()] * (parts + 1 + len(picks)),
        out_specs=[in_vmem()] * len(outs),
        out_shape=outs,
        scratch_shapes=[VMEM((hidden, parts * width), BF16)],
        compiler_params=pltpu.CompilerParams(vmem_limit_bytes=8 * 2**20),
        cost_estimate=pl.CostEstimate(flops=hidden * dense.size, bytes_accessed=dense.size, transcendentals=0),
    )(*blocks, dense, *picks)


def state_kernel(terms, *refs):
    flow = refs[0][...].astype(F32)
    for ref in refs[1:terms]:
        flow = flow + ref[...].astype(F32)
    mixing, base, out = refs[terms:]
    pre = base[...] + jnp.dot(mixing[...], flow.astype(BF16), preferred_element_type=F32)
    out[...] = jnp.tanh(pre).astype(BF16)


def adjoint_kernel(terms, *refs):
    back = refs[0][...].astype(F32)
    for ref in refs[1:terms]:
        back = back + ref[...].astype(F32)
    mixing, state, cotangent, out = refs[terms:]
    pulled = lax.dot_general(mixing[...], back.astype(BF16), TN, preferred_element_type=F32)
    wide = state[...].astype(F32)
    out[...] = ((1.0 - wide * wide) * (pulled + cotangent[...].astype(F32))).astype(BF16)


def finish(kernel, terms, others):
    return pl.pallas_call(
        functools.partial(kernel, len(terms)),
        in_specs=[in_vmem()] * (len(terms) + len(others)),
        out_specs=in_vmem(),
        out_shape=jax.ShapeDtypeStruct(terms[0].shape, BF16),
        compiler_params=pltpu.CompilerParams(vmem_limit_bytes=4 * 2**20),
        cost_estimate=pl.CostEstimate(flops=10**9, bytes_accessed=2**21, transcendentals=0),
    )(*terms, *others)


def per_device(state, adjoint, features, cotangent, mixing, input_weight, tiles, tile_rows, tile_cols, live_tiles):
    n_row, n_col = lax.axis_size("row"), lax.axis_size("col")
    hidden, nodes = state.shape
    slab = tiles[0, 0]
    side = slab.shape[-1]
    half_row, half_col = n_row // 2, n_col // 2
    piece = jax.ShapeDtypeStruct((hidden, nodes), BF16)
    wide = jax.ShapeDtypeStruct((hidden, nodes), F32)

    def by_row(value, mask):
        return swap(value, "row", n_row, mask)

    def by_col(value, mask):
        return swap(value, "col", n_col, mask)

    near = [adjoint]
    for k in range(1, half_row):
        far = k > 1 and k % 2
        near.append(by_row(near[k - 1] if far else adjoint, 2 if far else 2 * k))
    adjoints = []
    for block in near:
        adjoints += [block, by_row(block, 1)]

    near = [state] + [by_col(state, 2 * k) for k in range(1, half_col)]
    states = []
    for block in near:
        states += [block, by_col(block, 1)]

    blank = clear(n_col * nodes, n_row * nodes)
    dense = build(nodes // side, tile_rows, tile_cols, live_tiles, slab, blank)

    others = multiply(forward_kernel, states, dense, (), [piece] * half_row)
    direct = [by_row(others[1], 2)]
    crossed = {k: by_row(others[k], 1) for k in range(2, half_row)}
    mine = multiply(forward_kernel, states, dense, (input_weight, features), [piece] * half_row + [wide])
    *mine, base = mine
    direct.append(by_row(mine[1], 2))
    corner = (others[0].astype(F32) + direct[0].astype(F32)).astype(BF16)
    flows = [mine[0], direct[1], by_row(corner, 1)]
    relayed = None
    for k in reversed(range(2, half_row)):
        pair = mine[k].astype(F32) + crossed[k].astype(F32)
        if relayed is not None:
            pair = pair + relayed.astype(F32)
        far = k % 2
        moved = by_row(pair.astype(BF16), 2 if far else 2 * k)
        relayed = moved if far else None
        if not far:
            flows.append(moved)
    new_state = finish(state_kernel, flows, (mixing, base))

    others = multiply(backward_kernel, adjoints, dense, (), [piece] * half_col)
    others = [by_col(others[k], 1) for k in range(half_col)]
    mine = multiply(backward_kernel, adjoints, dense, others[1:], [piece] * half_col)
    backs = [mine[0], others[0]] + [by_col(mine[k], 2 * k) for k in range(1, half_col)]
    new_adjoint = finish(adjoint_kernel, backs, (mixing, state, cotangent))
    return (new_state, new_adjoint)


def solution(mesh):
    placed = (
        P(None, ("row", "col")),
        P(None, ("col", "row")),
        P(None, ("col", "row")),
        P(None, ("row", "col")),
        P(),
        P(),
        P("row", "col", None, None, None),
        P("row", "col", None),
        P("row", "col", None),
        P("row", "col"),
    )
    return jax.shard_map(
        per_device,
        mesh=mesh,
        in_specs=placed,
        out_specs=(P(None, ("col", "row")), P(None, ("row", "col"))),
        check_vma=False,
    )
```

```python
import functools

import jax
import jax.numpy as jnp
from jax import lax
from jax.experimental import pallas as pl
from jax.experimental.pallas import tpu as pltpu
from jax.sharding import PartitionSpec as P


VMEM = pltpu.VMEM
BF16 = jnp.bfloat16
F32 = jnp.float32
NT = (((1,), (1,)), ((), ()))
TN = (((0,), (0,)), ((), ()))


def in_vmem():
    return pl.BlockSpec(memory_space=VMEM)


def swap(value, axis, size, mask):
    return lax.ppermute(value, axis, [(i, i ^ mask) for i in range(size)])


def clear_kernel(dense):
    height, width = dense.shape

    def clear(i, carry):
        dense[pl.ds(pl.multiple_of(i * 32, 32), 32), :] = jnp.zeros((32, width), dense.dtype)
        return carry

    lax.fori_loop(0, height // 32, clear, 0)


def clear(height, width):
    return pl.pallas_call(
        clear_kernel,
        out_specs=in_vmem(),
        out_shape=jax.ShapeDtypeStruct((height, width), BF16),
        compiler_params=pltpu.CompilerParams(vmem_limit_bytes=4 * 2**20),
        cost_estimate=pl.CostEstimate(flops=5 * 10**9, bytes_accessed=height * width * 2, transcendentals=0),
        name="clear",
    )()


def build_kernel(per_chunk, rows, cols, count, tiles, blank, dense):
    slots, side, _ = tiles.shape
    row_flip = lax.axis_index("col") * per_chunk
    col_flip = lax.axis_index("row") * per_chunk

    def place(slot, carry):
        r = pl.multiple_of((rows[0, 0, slot] ^ row_flip) * side, side)
        c = pl.multiple_of((cols[0, 0, slot] ^ col_flip) * side, side)
        dense[pl.ds(r, side), pl.ds(c, side)] = tiles[slot]
        return carry

    lax.fori_loop(0, jnp.clip(count[0, 0], 0, slots), place, 0)


def build(per_chunk, rows, cols, count, tiles, blank):
    smem = pl.BlockSpec(memory_space=pltpu.SMEM)
    return pl.pallas_call(
        functools.partial(build_kernel, per_chunk),
        in_specs=[smem] * 3 + [in_vmem()] * 2,
        out_specs=in_vmem(),
        out_shape=jax.ShapeDtypeStruct(blank.shape, BF16),
        input_output_aliases={4: 0},
        compiler_params=pltpu.CompilerParams(vmem_limit_bytes=4 * 2**20),
        cost_estimate=pl.CostEstimate(flops=5 * 10**9, bytes_accessed=tiles.size * 2, transcendentals=0),
        name="build",
    )(rows, cols, count, tiles, blank)


def forward_kernel(parts, extra, cuts, *refs):
    blocks, dense, rest = refs[:parts], refs[parts], refs[parts + 1 :]
    picks, rest = rest[:extra], rest[extra:]
    outs, whole = rest[:-1], rest[-1]
    width = blocks[0].shape[1]
    for k in range(parts):
        whole[:, k * width : (k + 1) * width] = blocks[k][...]
    first = 1
    if extra:
        weight, features = picks
        outs[-1][...] = jnp.dot(weight[...], features[...], preferred_element_type=F32)
        outs, first = outs[:-1], 0
    span = outs[0].shape[1]
    for j, cut in enumerate(cuts):
        start = (2 * j + first) * span
        total = jnp.dot(
            whole[...], dense[:, start : start + span], preferred_element_type=F32
        ).astype(BF16)
        height = total.shape[0] // cut
        for i in range(cut):
            outs[i][...] = total[i * height : (i + 1) * height]
        outs = outs[cut:]


def early_kernel(parts, *refs):
    blocks, dense, outs, whole = refs[:parts], refs[parts], refs[parts + 1 : -1], refs[-1]
    width = blocks[0].shape[1]
    for k in range(parts):
        whole[:, k * width : (k + 1) * width] = blocks[k][...]
    span = outs[0].shape[1]
    for j, out in enumerate(outs):
        out[...] = lax.dot_general(
            whole[...], dense[j * span : (j + 1) * span, : parts * width], NT, preferred_element_type=F32
        )


def early(blocks, dense, pieces):
    hidden, width = blocks[0].shape
    parts = len(blocks)
    span = dense.shape[0] // pieces
    return pl.pallas_call(
        functools.partial(early_kernel, parts),
        in_specs=[in_vmem()] * (parts + 1),
        out_specs=[in_vmem()] * pieces,
        out_shape=[jax.ShapeDtypeStruct((hidden, span), F32)] * pieces,
        scratch_shapes=[VMEM((hidden, parts * width), BF16)],
        compiler_params=pltpu.CompilerParams(vmem_limit_bytes=8 * 2**20),
        cost_estimate=pl.CostEstimate(flops=2 * hidden * dense.size, bytes_accessed=dense.size, transcendentals=0),
        name="backward_early",
    )(*blocks, dense)


def late_kernel(first, terms, extra, *refs):
    block, dense, rest = refs[0], refs[1], refs[2:]
    sums, picks, outs = rest[:terms], rest[terms : terms + extra], rest[terms + extra :]
    span, width = outs[0].shape[1], block.shape[1]
    for j, out in enumerate(outs):
        start = (2 * j + first) * span
        total = sums[j][...] + lax.dot_general(
            block[...], dense[start : start + span, dense.shape[1] - width :], NT, preferred_element_type=F32
        )
        if extra and j:
            total = total + picks[j - 1][...].astype(F32)
        out[...] = total.astype(BF16)


def late(block, dense, first, sums, picks):
    hidden, width = block.shape
    span = sums[0].shape[1]
    return pl.pallas_call(
        functools.partial(late_kernel, first, len(sums), len(picks)),
        in_specs=[in_vmem()] * (2 + len(sums) + len(picks)),
        out_specs=[in_vmem()] * len(sums),
        out_shape=[jax.ShapeDtypeStruct((hidden, span), BF16)] * len(sums),
        compiler_params=pltpu.CompilerParams(vmem_limit_bytes=8 * 2**20),
        cost_estimate=pl.CostEstimate(flops=hidden * dense.shape[0] * width, bytes_accessed=dense.size // 8, transcendentals=0),
    )(block, dense, *sums, *picks)


def forward(blocks, dense, picks, cuts):
    hidden, width = blocks[0].shape
    parts = len(blocks)
    span = dense.shape[1] // (2 * len(cuts))
    outs = [jax.ShapeDtypeStruct((hidden // cut, span), BF16) for cut in cuts for _ in range(cut)]
    if picks:
        outs.append(jax.ShapeDtypeStruct((hidden, span), F32))
    outs = pl.pallas_call(
        functools.partial(forward_kernel, parts, len(picks), cuts),
        in_specs=[in_vmem()] * (parts + 1 + len(picks)),
        out_specs=[in_vmem()] * len(outs),
        out_shape=outs,
        scratch_shapes=[VMEM((hidden, parts * width), BF16)],
        compiler_params=pltpu.CompilerParams(vmem_limit_bytes=8 * 2**20),
        cost_estimate=pl.CostEstimate(flops=hidden * dense.size, bytes_accessed=dense.size, transcendentals=0),
    )(*blocks, dense, *picks)
    groups = []
    for cut in cuts:
        groups.append(outs[:cut])
        outs = outs[cut:]
    return groups, outs


def join_kernel(start, *refs):
    *terms, out = refs
    height = out.shape[0]
    total = None
    for ref in terms:
        value = ref[...] if ref.shape[0] == height else ref[start : start + height, :]
        value = value.astype(F32)
        total = value if total is None else total + value
    out[...] = total.astype(BF16)


def join(terms, start=0):
    return join_call(terms, start)


def join_call(terms, start):
    return pl.pallas_call(
        functools.partial(join_kernel, start),
        in_specs=[in_vmem()] * len(terms),
        out_specs=in_vmem(),
        out_shape=jax.ShapeDtypeStruct(terms[0].shape, BF16),
        compiler_params=pltpu.CompilerParams(vmem_limit_bytes=4 * 2**20),
        cost_estimate=pl.CostEstimate(flops=10**8, bytes_accessed=2**20, transcendentals=0),
        name="join",
    )(*terms)


def state_kernel(terms, pieces, *refs):
    flow = refs[0][...].astype(F32)
    for ref in refs[1:terms]:
        flow = flow + ref[...].astype(F32)
    for i in range(terms, terms + pieces, 2):
        flow = flow + jnp.concatenate([refs[i][...], refs[i + 1][...]], axis=0).astype(F32)
    mixing, base, out = refs[terms + pieces :]
    pre = base[...] + jnp.dot(mixing[...], flow.astype(BF16), preferred_element_type=F32)
    out[...] = jnp.tanh(pre).astype(BF16)


def adjoint_kernel(terms, pieces, *refs):
    back = refs[0][...].astype(F32)
    for ref in refs[1:terms]:
        back = back + ref[...].astype(F32)
    mixing, state, cotangent, out = refs[terms:]
    pulled = lax.dot_general(mixing[...], back.astype(BF16), TN, preferred_element_type=F32)
    wide = state[...].astype(F32)
    out[...] = ((1.0 - wide * wide) * (pulled + cotangent[...].astype(F32))).astype(BF16)


def finish(kernel, terms, halves, others):
    operands = (*terms, *halves, *others)
    return pl.pallas_call(
        functools.partial(kernel, len(terms), len(halves)),
        in_specs=[in_vmem()] * len(operands),
        out_specs=in_vmem(),
        out_shape=jax.ShapeDtypeStruct(terms[0].shape, BF16),
        compiler_params=pltpu.CompilerParams(vmem_limit_bytes=4 * 2**20),
        cost_estimate=pl.CostEstimate(flops=10**9, bytes_accessed=2**21, transcendentals=0),
    )(*operands)


def per_device(state, adjoint, features, cotangent, mixing, input_weight, tiles, tile_rows, tile_cols, live_tiles):
    n_row, n_col = lax.axis_size("row"), lax.axis_size("col")
    hidden, nodes = state.shape
    slab = tiles[0, 0]
    side = slab.shape[-1]
    half_row, half_col = n_row // 2, n_col // 2

    def by_row(value, mask):
        return swap(value, "row", n_row, mask)

    def by_col(value, mask):
        return swap(value, "col", n_col, mask)

    near = [adjoint]
    for k in range(1, half_row):
        far = k > 1 and k % 2
        near.append(by_row(near[k - 1] if far else adjoint, 2 if far else 2 * k))
    adjoints = []
    for block in near:
        adjoints += [block, by_row(block, 1)]

    near = [state] + [by_col(state, 2 * k) for k in range(1, half_col)]
    states = []
    for block in near:
        states += [block, by_col(block, 1)]

    blank = clear(n_col * nodes, n_row * nodes)
    dense = build(nodes // side, tile_rows, tile_cols, live_tiles, slab, blank)

    cuts = [2 if k > 1 and k % 2 == 0 else 1 for k in range(half_row)]
    others, _ = forward(states, dense, (), cuts)
    direct = by_row(others[1][0], 2)
    crossed = {k: [by_row(part, 1) for part in others[k]] for k in range(2, half_row)}
    mine, (base,) = forward(states, dense, (input_weight, features), cuts)
    corner = join((others[0][0], direct))
    flows = [mine[0][0], by_row(mine[1][0], 2), by_row(corner, 1)]
    halves, relayed = [], None
    for k in reversed(range(2, half_row)):
        if k % 2:
            relayed = by_row(join((mine[k][0], crossed[k][0])), 2)
            continue
        last = () if relayed is None else (relayed,)
        for i in range(2):
            pair = join((mine[k][i], crossed[k][i], *last), i * hidden // 2)
            halves.append(by_row(pair, 2 * k))
        relayed = None
    new_state = finish(state_kernel, flows, halves, (mixing, base))

    sums = early(adjoints[:-1], dense, n_col)
    others = late(adjoints[-1], dense, 1, sums[1::2], ())
    others = [by_col(others[k], 1) for k in range(half_col)]
    mine = late(adjoints[-1], dense, 0, sums[::2], others[1:])
    backs = [mine[0], others[0]] + [by_col(mine[k], 2 * k) for k in range(1, half_col)]
    new_adjoint = finish(adjoint_kernel, backs, (), (mixing, state, cotangent))
    return (new_state, new_adjoint)


def solution(mesh):
    placed = (
        P(None, ("row", "col")),
        P(None, ("col", "row")),
        P(None, ("col", "row")),
        P(None, ("row", "col")),
        P(),
        P(),
        P("row", "col", None, None, None),
        P("row", "col", None),
        P("row", "col", None),
        P("row", "col"),
    )
    return jax.shard_map(
        per_device,
        mesh=mesh,
        in_specs=placed,
        out_specs=(P(None, ("col", "row")), P(None, ("row", "col"))),
        check_vma=False,
    )
```

```python
import functools

import jax
import jax.numpy as jnp
from jax import lax
from jax.experimental import pallas as pl
from jax.experimental.pallas import tpu as pltpu
from jax.sharding import PartitionSpec as P


VMEM = pltpu.VMEM
BF16 = jnp.bfloat16
F32 = jnp.float32
NT = (((1,), (1,)), ((), ()))
TN = (((0,), (0,)), ((), ()))


def in_vmem():
    return pl.BlockSpec(memory_space=VMEM)


def swap(value, axis, size, mask):
    return lax.ppermute(value, axis, [(i, i ^ mask) for i in range(size)])


def clear_kernel(dense):
    height, width = dense.shape

    def clear(i, carry):
        dense[pl.ds(pl.multiple_of(i * 32, 32), 32), :] = jnp.zeros((32, width), dense.dtype)
        return carry

    lax.fori_loop(0, height // 32, clear, 0)


def clear(height, width):
    return pl.pallas_call(
        clear_kernel,
        out_specs=in_vmem(),
        out_shape=jax.ShapeDtypeStruct((height, width), BF16),
        compiler_params=pltpu.CompilerParams(vmem_limit_bytes=4 * 2**20),
        cost_estimate=pl.CostEstimate(flops=5 * 10**9, bytes_accessed=height * width * 2, transcendentals=0),
        name="clear",
    )()


def build_kernel(per_chunk, rows, cols, count, tiles, blank, dense):
    slots, side, _ = tiles.shape
    row_flip = lax.axis_index("col") * per_chunk
    col_flip = lax.axis_index("row") * per_chunk

    def place(slot, carry):
        r = pl.multiple_of((rows[0, 0, slot] ^ row_flip) * side, side)
        c = pl.multiple_of((cols[0, 0, slot] ^ col_flip) * side, side)
        dense[pl.ds(r, side), pl.ds(c, side)] = tiles[slot]
        return carry

    lax.fori_loop(0, jnp.clip(count[0, 0], 0, slots), place, 0)


def build(per_chunk, rows, cols, count, tiles, blank):
    smem = pl.BlockSpec(memory_space=pltpu.SMEM)
    return pl.pallas_call(
        functools.partial(build_kernel, per_chunk),
        in_specs=[smem] * 3 + [in_vmem()] * 2,
        out_specs=in_vmem(),
        out_shape=jax.ShapeDtypeStruct(blank.shape, BF16),
        input_output_aliases={4: 0},
        compiler_params=pltpu.CompilerParams(vmem_limit_bytes=4 * 2**20),
        cost_estimate=pl.CostEstimate(flops=5 * 10**9, bytes_accessed=tiles.size * 2, transcendentals=0),
        name="build",
    )(rows, cols, count, tiles, blank)


def forward_kernel(parts, extra, cuts, *refs):
    blocks, dense, rest = refs[:parts], refs[parts], refs[parts + 1 :]
    picks, rest = rest[:extra], rest[extra:]
    outs, whole = rest[:-1], rest[-1]
    width = blocks[0].shape[1]
    for k in range(parts):
        whole[:, k * width : (k + 1) * width] = blocks[k][...]
    first = 1
    if extra:
        weight, features = picks
        outs[-1][...] = jnp.dot(weight[...], features[...], preferred_element_type=F32)
        outs, first = outs[:-1], 0
    span = outs[0].shape[1]
    for j, cut in enumerate(cuts):
        start = (2 * j + first) * span
        total = jnp.dot(
            whole[...], dense[:, start : start + span], preferred_element_type=F32
        ).astype(BF16)
        height = total.shape[0] // cut
        for i in range(cut):
            outs[i][...] = total[i * height : (i + 1) * height]
        outs = outs[cut:]


def early_kernel(parts, *refs):
    blocks, dense, outs, whole = refs[:parts], refs[parts], refs[parts + 1 : -1], refs[-1]
    width = blocks[0].shape[1]
    for k in range(parts):
        whole[:, k * width : (k + 1) * width] = blocks[k][...]
    span = outs[0].shape[1]
    for j, out in enumerate(outs):
        out[...] = lax.dot_general(
            whole[...], dense[j * span : (j + 1) * span, : parts * width], NT, preferred_element_type=F32
        )


def early(blocks, dense, pieces):
    hidden, width = blocks[0].shape
    parts = len(blocks)
    span = dense.shape[0] // pieces
    return pl.pallas_call(
        functools.partial(early_kernel, parts),
        in_specs=[in_vmem()] * (parts + 1),
        out_specs=[in_vmem()] * pieces,
        out_shape=[jax.ShapeDtypeStruct((hidden, span), F32)] * pieces,
        scratch_shapes=[VMEM((hidden, parts * width), BF16)],
        compiler_params=pltpu.CompilerParams(vmem_limit_bytes=8 * 2**20),
        cost_estimate=pl.CostEstimate(flops=2 * hidden * dense.size, bytes_accessed=dense.size, transcendentals=0),
        name="backward_early",
    )(*blocks, dense)


def late_kernel(first, terms, extra, *refs):
    block, dense, rest = refs[0], refs[1], refs[2:]
    sums, picks, outs = rest[:terms], rest[terms : terms + extra], rest[terms + extra :]
    span, width = outs[0].shape[1], block.shape[1]
    for j, out in enumerate(outs):
        start = (2 * j + first) * span
        total = sums[j][...] + lax.dot_general(
            block[...], dense[start : start + span, dense.shape[1] - width :], NT, preferred_element_type=F32
        )
        if extra and j:
            total = total + picks[j - 1][...].astype(F32)
        out[...] = total.astype(BF16)


def late(block, dense, first, sums, picks):
    hidden, width = block.shape
    span = sums[0].shape[1]
    return pl.pallas_call(
        functools.partial(late_kernel, first, len(sums), len(picks)),
        in_specs=[in_vmem()] * (2 + len(sums) + len(picks)),
        out_specs=[in_vmem()] * len(sums),
        out_shape=[jax.ShapeDtypeStruct((hidden, span), BF16)] * len(sums),
        compiler_params=pltpu.CompilerParams(vmem_limit_bytes=8 * 2**20),
        cost_estimate=pl.CostEstimate(flops=hidden * dense.shape[0] * width, bytes_accessed=dense.size // 8, transcendentals=0),
    )(block, dense, *sums, *picks)


def forward(blocks, dense, picks, cuts):
    hidden, width = blocks[0].shape
    parts = len(blocks)
    span = dense.shape[1] // (2 * len(cuts))
    outs = [jax.ShapeDtypeStruct((hidden // cut, span), BF16) for cut in cuts for _ in range(cut)]
    if picks:
        outs.append(jax.ShapeDtypeStruct((hidden, span), F32))
    outs = pl.pallas_call(
        functools.partial(forward_kernel, parts, len(picks), cuts),
        in_specs=[in_vmem()] * (parts + 1 + len(picks)),
        out_specs=[in_vmem()] * len(outs),
        out_shape=outs,
        scratch_shapes=[VMEM((hidden, parts * width), BF16)],
        compiler_params=pltpu.CompilerParams(vmem_limit_bytes=8 * 2**20),
        cost_estimate=pl.CostEstimate(flops=hidden * dense.size, bytes_accessed=dense.size, transcendentals=0),
    )(*blocks, dense, *picks)
    groups = []
    for cut in cuts:
        groups.append(outs[:cut])
        outs = outs[cut:]
    return groups, outs


def join_kernel(first, second, out):
    out[...] = (first[...].astype(F32) + second[...].astype(F32)).astype(BF16)


def join(terms):
    return pl.pallas_call(
        join_kernel,
        in_specs=[in_vmem()] * 2,
        out_specs=in_vmem(),
        out_shape=jax.ShapeDtypeStruct(terms[0].shape, BF16),
        compiler_params=pltpu.CompilerParams(vmem_limit_bytes=4 * 2**20),
        cost_estimate=pl.CostEstimate(flops=10**8, bytes_accessed=2**20, transcendentals=0),
        name="join",
    )(*terms)


def state_kernel(terms, pieces, *refs):
    flow = refs[0][...].astype(F32)
    for ref in refs[1:terms]:
        flow = flow + ref[...].astype(F32)
    for i in range(terms, terms + pieces, 2):
        flow = flow + jnp.concatenate([refs[i][...], refs[i + 1][...]], axis=0).astype(F32)
    mixing, base, out = refs[terms + pieces :]
    pre = base[...] + jnp.dot(mixing[...], flow.astype(BF16), preferred_element_type=F32)
    out[...] = jnp.tanh(pre).astype(BF16)


def adjoint_kernel(terms, pieces, *refs):
    back = refs[0][...].astype(F32)
    for ref in refs[1:terms]:
        back = back + ref[...].astype(F32)
    mixing, state, cotangent, out = refs[terms:]
    pulled = lax.dot_general(mixing[...], back.astype(BF16), TN, preferred_element_type=F32)
    wide = state[...].astype(F32)
    out[...] = ((1.0 - wide * wide) * (pulled + cotangent[...].astype(F32))).astype(BF16)


def finish(kernel, terms, halves, others):
    operands = (*terms, *halves, *others)
    return pl.pallas_call(
        functools.partial(kernel, len(terms), len(halves)),
        in_specs=[in_vmem()] * len(operands),
        out_specs=in_vmem(),
        out_shape=jax.ShapeDtypeStruct(terms[0].shape, BF16),
        compiler_params=pltpu.CompilerParams(vmem_limit_bytes=4 * 2**20),
        cost_estimate=pl.CostEstimate(flops=10**9, bytes_accessed=2**21, transcendentals=0),
    )(*operands)


def per_device(state, adjoint, features, cotangent, mixing, input_weight, tiles, tile_rows, tile_cols, live_tiles):
    n_row, n_col = lax.axis_size("row"), lax.axis_size("col")
    _, nodes = state.shape
    slab = tiles[0, 0]
    side = slab.shape[-1]
    half_row, half_col = n_row // 2, n_col // 2

    def by_row(value, mask):
        return swap(value, "row", n_row, mask)

    def by_col(value, mask):
        return swap(value, "col", n_col, mask)

    near = [adjoint]
    for k in range(1, half_row):
        far = k > 1 and k % 2
        near.append(by_row(near[k - 1] if far else adjoint, 2 if far else 2 * k))
    adjoints = []
    for block in near:
        adjoints += [block, by_row(block, 1)]

    near = [state] + [by_col(state, 2 * k) for k in range(1, half_col)]
    states = []
    for block in near:
        states += [block, by_col(block, 1)]

    blank = clear(n_col * nodes, n_row * nodes)
    dense = build(nodes // side, tile_rows, tile_cols, live_tiles, slab, blank)

    cuts = [2 if k > 1 and k % 2 == 0 else 1 for k in range(half_row)]
    others, _ = forward(states, dense, (), cuts)
    direct = by_row(others[1][0], 2)
    crossed = {k: [by_row(part, 1) for part in others[k]] for k in range(2, half_row)}
    mine, (base,) = forward(states, dense, (input_weight, features), cuts)
    corner = join((others[0][0], direct))
    flows = [mine[0][0], by_row(mine[1][0], 2), by_row(corner, 1)]
    halves = []
    for k in reversed(range(2, half_row)):
        if k % 2:
            flows.append(by_row(join((mine[k][0], crossed[k][0])), 2 * k))
            continue
        for i in range(2):
            pair = join((mine[k][i], crossed[k][i]))
            halves.append(by_row(pair, 2 * k))
    new_state = finish(state_kernel, flows, halves, (mixing, base))

    sums = early(adjoints[:-1], dense, n_col)
    others = late(adjoints[-1], dense, 1, sums[1::2], ())
    others = [by_col(others[k], 1) for k in range(half_col)]
    mine = late(adjoints[-1], dense, 0, sums[::2], others[1:])
    backs = [mine[0], others[0]] + [by_col(mine[k], 2 * k) for k in range(1, half_col)]
    new_adjoint = finish(adjoint_kernel, backs, (), (mixing, state, cotangent))
    return (new_state, new_adjoint)


def solution(mesh):
    placed = (
        P(None, ("row", "col")),
        P(None, ("col", "row")),
        P(None, ("col", "row")),
        P(None, ("row", "col")),
        P(),
        P(),
        P("row", "col", None, None, None),
        P("row", "col", None),
        P("row", "col", None),
        P("row", "col"),
    )
    return jax.shard_map(
        per_device,
        mesh=mesh,
        in_specs=placed,
        out_specs=(P(None, ("col", "row")), P(None, ("row", "col"))),
        check_vma=False,
    )
```
